32 devices in a mesh: seq: 8 (over z, x), head: 4 (over y, core).
Axes of the slice: x: 2, y: 2, z: 4, core: 2. Of those that a mesh axis runs over, the one named last changes fastest.
Arguments:
- patches: bfloat16 [32768, 768], P('seq'), may hold values from -6 to 6
- slot_image: int32 [128], P('seq'), may hold values from -1 to 63, as said below
- slot_dest: int32 [128], P('seq'), may hold values from -1 to 63, as said below
- enc_gain: float32 [768], replicated, may hold values from 0.1 to 1.9
- w_qkv: bfloat16 [3, 768, 768], P(None, None, 'head'), may hold values from -1.2 to 1.2
- w_out: bfloat16 [768, 768], P('head'), may hold values from -0.21875 to 0.21875
- fast_gain: float32 [768], replicated, may hold values from 0.1 to 1.9
- w_fast: bfloat16 [3, 768, 768], P(None, None, 'head'), may hold values from -0.21875 to 0.21875
- w_rate: bfloat16 [768, 4], P(None, 'head'), may hold values from -0.21875 to 0.21875
- fast_gate_up: float32 [4, 2, 192, 384], P('head'), may hold values from -0.4375 to 0.4375
- fast_down: float32 [4, 384, 192], P('head'), may hold values from -0.3125 to 0.3125
Outputs:
- view_out: bfloat16 [16384, 768], P('seq', 'head')
The draws below stay inside these ranges and needn't reach their ends.
Inputs may be any that keep to these rules, and one draw needn't show every extreme that they name: slot_dest gives for each slot the view-order block that its block becomes, or -1 for an empty slot; every view-order block is named by exactly one slot. Slots 2i and 2i + 1 of one seq index are both empty or name view blocks 2m and 2m + 1. The slots of one seq index name at most 2 blocks of any one view shard (blocks s * 8 to (s + 1) * 8 - 1), and some seq index uses all of its slots. slot_image is -1 exactly where slot_dest is -1; an image is one block or the two blocks of a slot pair, and different images have different ids.
All inputs are finite; a program needn't handle non-finite values.
Results may differ from the reference program's by a relative error of at most 0.035.
Values may be sent and summed in bfloat16 or wider, within the bound.
A program may use at most 128 MiB of HBM per device.

```python
import math
import jax
import jax.numpy as jnp
from jax import lax

D = 768
HDIM = 64
FHEADS = 4
FW = 192
FH = 384
BLK = 256
BLK_DEV = 8
WSLOT = 16
VTOKENS = 16384
WTOKENS = 32768
N_SEQ = 8


def source_rank(source, busiest):
    half_away = (busiest + N_SEQ // 2) % N_SEQ
    next_one = (busiest + 1) % N_SEQ
    rotated = (source - busiest - 2) % N_SEQ
    rest = jnp.where(rotated < N_SEQ // 2 - 2, rotated + 2, rotated + 1)
    return jnp.where(source == half_away, 0, jnp.where(source == next_one, 1, rest))


def slot_layout(key):
    key_parts = jax.random.split(jax.random.fold_in(key, 41), 5)
    bins_dev = BLK_DEV // 2
    busiest = jax.random.randint(key_parts[0], (), 0, N_SEQ)
    shifts = jax.random.permutation(key_parts[2], N_SEQ - 1)
    paired = jax.random.randint(key_parts[3], (N_SEQ, bins_dev), 0, 2)
    places = jax.vmap(lambda part_key: jax.random.permutation(part_key, BLK_DEV))(jax.random.split(key_parts[4], N_SEQ))
    source = jnp.broadcast_to(jnp.arange(N_SEQ, dtype=jnp.int32)[:, None], (N_SEQ, bins_dev))
    column = jnp.broadcast_to(jnp.arange(bins_dev, dtype=jnp.int32)[None, :], (N_SEQ, bins_dev))
    ordinal = column * N_SEQ + source_rank(source, busiest)
    to_busiest = ordinal < BLK_DEV
    offset_bin = shifts[column % (N_SEQ - 1)]
    spread_to = (busiest + 1 + (source + offset_bin) % (N_SEQ - 1)) % N_SEQ
    worker = jnp.where(to_busiest, busiest, spread_to)
    place_bin = jnp.where(to_busiest, ordinal, 2 * column + (source == N_SEQ - 1).astype(jnp.int32))
    place_bin = places[worker, place_bin]
    view_first = source * BLK_DEV + 2 * column
    slot_first = worker * (2 * BLK_DEV) + 2 * place_bin
    second_image = jnp.where(paired == 1, view_first, view_first + 1)
    slot_all = jnp.concatenate([slot_first.reshape(-1), slot_first.reshape(-1) + 1]).astype(jnp.int32)
    view_all = jnp.concatenate([view_first.reshape(-1), view_first.reshape(-1) + 1]).astype(jnp.int32)
    image_all = jnp.concatenate([view_first.reshape(-1), second_image.reshape(-1)]).astype(jnp.int32)
    unused = jnp.full((N_SEQ * 2 * BLK_DEV,), -1, jnp.int32)
    return (unused.at[slot_all].set(image_all), unused.at[slot_all].set(view_all))


def draw_slot_image(key, part):
    return slot_layout(key)[0]


def draw_slot_dest(key, part):
    return slot_layout(key)[1]


def draw_w_qkv(key, part):
    key_parts = jax.random.split(jax.random.fold_in(key, 77), 1)
    spread = D ** (-0.5)
    weights = jax.random.normal(key_parts[0], (3, D, D), jnp.float32) * spread
    return jnp.clip(weights, -1.15, 1.15).astype(jnp.bfloat16)


def block_scale(own_key, shape, cuts, smallest, largest):
    factor_of = 1.0
    for position, shards_of in cuts:
        steps = jax.random.uniform(jax.random.fold_in(jax.random.fold_in(own_key, 6), position), (shards_of,), jnp.float32, smallest / len(cuts), largest / len(cuts))
        factor_of = factor_of * jnp.repeat(jnp.exp(steps), shape[position] // shards_of).reshape((-1,) + (1,) * (len(shape) - 1 - position))
    return factor_of


def scatter_about(rng, shape, scale, reach, shards=(), kind=jnp.bfloat16):
    array = scale * jax.random.normal(rng, shape, jnp.float32)
    if shards:
        array = array * block_scale(rng, shape, shards, -0.22, 0.18)
    return jnp.clip(array, -reach, reach).astype(kind)


def setup_inputs(seed: int = 0) -> dict:
    seeds = jax.random.split(jax.random.key(seed), 12)
    return {
        "patches": scatter_about(seeds[0], (WTOKENS, D), 1.0, 6.0, ((0, 8),)),
        "slot_image": draw_slot_image(jax.random.fold_in(seeds[11], 71), 0),
        "slot_dest": draw_slot_dest(jax.random.fold_in(seeds[11], 71), 0),
        "enc_gain": jnp.clip(1.0 + 0.18 * jax.random.normal(seeds[3], (D,), jnp.float32), 0.1, 1.9),
        "w_qkv": draw_w_qkv(jax.random.fold_in(seeds[11], 71), 0),
        "w_out": scatter_about(seeds[5], (D, D), D ** -0.5, 0.21875, ((0, 4),)),
        "fast_gain": jnp.clip(1.0 + 0.18 * jax.random.normal(seeds[6], (D,), jnp.float32), 0.1, 1.9),
        "w_fast": scatter_about(seeds[7], (3, D, D), D ** -0.5, 0.21875, ((2, 4),)),
        "w_rate": scatter_about(seeds[8], (D, FHEADS), D ** -0.5, 0.21875, ((1, 4),)),
        "fast_gate_up": scatter_about(seeds[9], (FHEADS, 2, FW, FH), FW ** -0.5, 0.4375, ((0, 4),), jnp.float32),
        "fast_down": scatter_about(seeds[10], (FHEADS, FH, FW), FH ** -0.5, 0.3125, ((0, 4),), jnp.float32),
    }


EPSILON = 1e-06
RATE_SCALE = 0.1

def norm_rows(values, gain_vector):
    widened = values.astype(jnp.float32)
    factor = lax.rsqrt(lax.optimization_barrier(jnp.mean(widened * widened, axis=-1, keepdims=True)) + EPSILON)
    return (widened * factor * gain_vector.astype(jnp.float32)).astype(jnp.bfloat16)

def attend_pair(pieces):
    query_rows, key_rows, value_rows, token_ids = pieces
    token_count = query_rows.shape[0]
    heads_here = query_rows.shape[1] // HDIM
    q_heads = query_rows.astype(jnp.float32).reshape(token_count, heads_here, HDIM)
    k_heads = key_rows.astype(jnp.float32).reshape(token_count, heads_here, HDIM)
    v_heads = value_rows.astype(jnp.float32).reshape(token_count, heads_here, HDIM)
    scores = jnp.einsum('qhe,khe->hqk', q_heads, k_heads) * HDIM ** (-0.5)
    allowed = token_ids[:, None] == token_ids[None, :]
    scores = jnp.where(allowed[None], scores, -1e+30)
    top_score = lax.optimization_barrier(jnp.max(scores, axis=-1, keepdims=True))
    exp_scores = jnp.exp(scores - top_score)
    weights = (exp_scores / lax.optimization_barrier(jnp.sum(exp_scores, axis=-1, keepdims=True))).astype(jnp.bfloat16)
    mixed_heads = jnp.einsum('hqk,khe->qhe', weights.astype(jnp.float32), v_heads)
    return mixed_heads.astype(jnp.bfloat16).reshape(token_count, heads_here * HDIM)

def encode_group(rows_here, ids_here, enc_gain, w_qkv, w_out):
    normed = norm_rows(rows_here, enc_gain)
    projected = [jnp.dot(normed, w_qkv[which_one], preferred_element_type=jnp.float32).astype(jnp.bfloat16) for which_one in range(3)]
    span = 2 * BLK
    pair_count = rows_here.shape[0] // span
    attended = lax.map(attend_pair, (projected[0].reshape(pair_count, span, D), projected[1].reshape(pair_count, span, D), projected[2].reshape(pair_count, span, D), ids_here.reshape(pair_count, span)))
    attended = attended.reshape(rows_here.shape[0], D)
    head_total = jnp.zeros((rows_here.shape[0], D), jnp.float32)
    for group_index in range(FHEADS):
        block_cols = attended[:, group_index * FW:(group_index + 1) * FW]
        product = jnp.dot(block_cols, w_out[group_index * FW:(group_index + 1) * FW], preferred_element_type=jnp.float32)
        rounded = lax.optimization_barrier(product.astype(jnp.bfloat16))
        head_total = head_total + rounded.astype(jnp.float32)
    return (rows_here.astype(jnp.float32) + head_total).astype(jnp.bfloat16)

def renorm(updated, initial):
    target_norm = jnp.sqrt(lax.optimization_barrier(jnp.sum(initial * initial, axis=1, keepdims=True)))
    return updated * target_norm * lax.rsqrt(lax.optimization_barrier(jnp.sum(updated * updated, axis=1, keepdims=True)) + EPSILON)

def reference(patches, slot_image, slot_dest, enc_gain, w_qkv, w_out, fast_gain, w_fast, w_rate, fast_gate_up, fast_down):
    view_count = N_SEQ * BLK_DEV
    slot_total = N_SEQ * WSLOT
    target = jnp.where(slot_dest >= 0, slot_dest, view_count).astype(jnp.int32)
    view_blocks = jnp.zeros((view_count + 1, BLK, D), patches.dtype).at[target].set(patches.reshape(slot_total, BLK, D))[:view_count]
    view_ids = jnp.zeros((view_count + 1,), jnp.int32).at[target].set(slot_image.astype(jnp.int32))[:view_count]
    pair_total = view_count // 2
    group_size = math.gcd(8, pair_total)
    group_rows = view_blocks.reshape(pair_total // group_size, group_size * 2 * BLK, D)
    group_ids = jnp.repeat(view_ids, BLK).reshape(pair_total // group_size, group_size * 2 * BLK)
    embedded = lax.map(lambda pieces: encode_group(pieces[0], pieces[1], enc_gain, w_qkv, w_out), (group_rows, group_ids))
    embedded = embedded.reshape(view_count * BLK, D)
    normed_fast = norm_rows(embedded, fast_gain)
    fast_query = jnp.dot(normed_fast, w_fast[0], preferred_element_type=jnp.float32).astype(jnp.bfloat16)
    fast_key = jnp.dot(normed_fast, w_fast[1], preferred_element_type=jnp.float32).astype(jnp.bfloat16)
    fast_value = jnp.dot(normed_fast, w_fast[2], preferred_element_type=jnp.float32).astype(jnp.bfloat16)
    rate_all = RATE_SCALE * jax.nn.softplus(jnp.dot(normed_fast, w_rate, preferred_element_type=jnp.float32)) * VTOKENS ** (-0.5)
    columns_out = []
    for fast_head in range(FHEADS):
        chosen = slice(fast_head * FW, (fast_head + 1) * FW)
        key_here = fast_key[:, chosen]
        query_here = fast_query[:, chosen]
        gate_init = fast_gate_up[fast_head, 0]
        up_init = fast_gate_up[fast_head, 1]
        down_init = fast_down[fast_head]
        gate_half = gate_init.astype(jnp.bfloat16)
        up_half = up_init.astype(jnp.bfloat16)
        down_half = down_init.astype(jnp.bfloat16)
        key_gate = jnp.dot(key_here, gate_half, preferred_element_type=jnp.float32)
        key_up = jnp.dot(key_here, up_half, preferred_element_type=jnp.float32)
        hidden_key = (jax.nn.silu(key_gate) * key_up).astype(jnp.bfloat16)
        out_grad = (-rate_all[:, fast_head:fast_head + 1] * fast_value[:, chosen].astype(jnp.float32)).astype(jnp.bfloat16)
        grad_down = jnp.dot(hidden_key.T, out_grad, preferred_element_type=jnp.float32)
        hidden_grad = jnp.dot(out_grad, down_half.T, preferred_element_type=jnp.float32)
        sigmoid_gate = jax.nn.sigmoid(key_gate)
        gate_grad = (hidden_grad * key_up * sigmoid_gate * (1.0 + key_gate * (1.0 - sigmoid_gate))).astype(jnp.bfloat16)
        up_grad = (hidden_grad * jax.nn.silu(key_gate)).astype(jnp.bfloat16)
        grad_gate = jnp.dot(key_here.T, gate_grad, preferred_element_type=jnp.float32)
        grad_up = jnp.dot(key_here.T, up_grad, preferred_element_type=jnp.float32)
        applied_gate = renorm(gate_init - grad_gate, gate_init).astype(jnp.bfloat16)
        applied_up = renorm(up_init - grad_up, up_init).astype(jnp.bfloat16)
        applied_down = renorm(down_init - grad_down, down_init).astype(jnp.bfloat16)
        query_gate = jnp.dot(query_here, applied_gate, preferred_element_type=jnp.float32)
        query_up = jnp.dot(query_here, applied_up, preferred_element_type=jnp.float32)
        query_hidden = (jax.nn.silu(query_gate) * query_up).astype(jnp.bfloat16)
        fast_out = jnp.dot(query_hidden, applied_down, preferred_element_type=jnp.float32)
        columns_out.append((embedded[:, chosen].astype(jnp.float32) + fast_out).astype(jnp.bfloat16))
    return jnp.concatenate(columns_out, axis=1)
```

```python
import functools

import jax
import jax.numpy as jnp
from jax import lax
from jax.experimental import pallas as pl
from jax.experimental.pallas import tpu as pltpu
from jax.sharding import PartitionSpec as P

HDIM = 64
BLK = 256
BLK_DEV = 8
PAIR = 2 * BLK
EPSILON = 1e-06
RATE_SCALE = 0.1
LANES = 128
MESH = pl.DeviceIdType.MESH
VMEM = pl.BlockSpec(memory_space=pltpu.VMEM)
NT = (((1,), (1,)), ((), ()))


def remote(src, dst, send, recv, device):
    return pltpu.make_async_remote_copy(
        src_ref=src, dst_ref=dst, send_sem=send, recv_sem=recv, device_id=device, device_id_type=MESH
    )


def comm_params(number):
    return pltpu.CompilerParams(
        collective_id=number, has_side_effects=True, vmem_limit_bytes=56 * 1024 * 1024
    )


def greet(devices):
    barrier = pltpu.get_barrier_semaphore()
    for device in devices:
        pl.semaphore_signal(barrier, inc=1, device_id=device, device_id_type=MESH)
    pl.semaphore_wait(barrier, len(devices))


def others(axis_size, me):
    return [lax.rem(me + step, axis_size) for step in range(1, axis_size)]


def head_pals(head_count, head):
    partner = head + 1 - 2 * lax.rem(head, 2)
    peer = lax.rem(head + head_count // 2, head_count)
    return partner, peer


def entry_kernel(n, nh, x_ref, m_ref, w_ref, ox, om, ow, sx, rx, sm, rm, sw, rw):
    seq, head = lax.axis_index("seq"), lax.axis_index("head")
    partner, peer = head_pals(nh, head)
    across = lax.rem(partner + nh // 2, nh)
    targets = others(n, seq)
    greet([(seq, partner), (seq, peer)] + [(to, head) for to in targets])
    to_peer = remote(w_ref, ow.at[:, head], sw.at[0], rw.at[0], (seq, peer))
    to_partner = remote(w_ref, ow.at[:, head], sw.at[1], rw.at[1], (seq, partner))
    to_peer.start()
    to_partner.start()
    copies = []
    for step, to in enumerate(targets):
        copies.append(remote(m_ref.at[to], om.at[seq], sm.at[step], rm.at[step], (to, head)))
        copies.append(remote(x_ref.at[to], ox.at[seq], sx.at[step], rx.at[step], (to, head)))
    for copy in copies:
        copy.start()
    ox[seq] = x_ref[seq]
    om[seq] = m_ref[seq]
    for part in range(w_ref.shape[0]):
        ow[part, head] = w_ref[part]
    to_peer.wait_recv()
    forward = remote(ow.at[:, peer], ow.at[:, peer], sw.at[2], rw.at[2], (seq, partner))
    forward.start()
    to_peer.wait_send()
    to_partner.wait()
    for copy in copies:
        copy.wait()
    forward.wait()


def enter(rows, meta, weights, n, nh):
    dma = pltpu.SemaphoreType.DMA
    return pl.pallas_call(
        functools.partial(entry_kernel, n, nh),
        out_shape=(
            jax.ShapeDtypeStruct(rows.shape, rows.dtype),
            jax.ShapeDtypeStruct(meta.shape, meta.dtype),
            jax.ShapeDtypeStruct(
                (weights.shape[0], nh) + weights.shape[1:], weights.dtype
            ),
        ),
        in_specs=[VMEM] * 3,
        out_specs=(VMEM,) * 3,
        scratch_shapes=[
            dma((n - 1,)), dma((n - 1,)), dma((n - 1,)), dma((n - 1,)), dma((3,)), dma((3,)),
        ],
        compiler_params=comm_params(1),
        name="entry_exchange",
    )(rows, meta, weights)


def swap_kernel(nh, x_ref, o_ref, send, recv):
    seq, head = lax.axis_index("seq"), lax.axis_index("head")
    targets = others(nh, head)
    greet([(seq, to) for to in targets])
    copies = [
        remote(x_ref.at[to], o_ref.at[head], send.at[step], recv.at[step], (seq, to))
        for step, to in enumerate(targets)
    ]
    for copy in copies:
        copy.start()
    o_ref[head] = x_ref[head]
    for copy in copies:
        copy.wait()


def head_swap(x, nh):
    dma = pltpu.SemaphoreType.DMA
    return pl.pallas_call(
        functools.partial(swap_kernel, nh),
        out_shape=jax.ShapeDtypeStruct(x.shape, x.dtype),
        in_specs=[VMEM],
        out_specs=VMEM,
        scratch_shapes=[dma((nh - 1,)), dma((nh - 1,))],
        compiler_params=comm_params(2),
        name="head_swap",
    )(x)


def gather_kernel(nh, x_ref, o_ref, send, recv):
    seq, head = lax.axis_index("seq"), lax.axis_index("head")
    partner, peer = head_pals(nh, head)
    greet([(seq, partner), (seq, peer)])
    to_peer = remote(x_ref, o_ref.at[head], send.at[0], recv.at[0], (seq, peer))
    to_partner = remote(x_ref, o_ref.at[head], send.at[1], recv.at[1], (seq, partner))
    to_peer.start()
    to_partner.start()
    o_ref[head] = x_ref[...]
    to_peer.wait_recv()
    forward = remote(o_ref.at[peer], o_ref.at[peer], send.at[2], recv.at[2], (seq, partner))
    forward.start()
    to_peer.wait_send()
    to_partner.wait()
    forward.wait()


def head_gather(x, nh):
    dma = pltpu.SemaphoreType.DMA
    return pl.pallas_call(
        functools.partial(gather_kernel, nh),
        out_shape=jax.ShapeDtypeStruct((nh,) + x.shape, x.dtype),
        in_specs=[VMEM],
        out_specs=VMEM,
        scratch_shapes=[dma((3,)), dma((3,))],
        compiler_params=comm_params(3),
        name="head_gather",
    )(x)


def sum_kernel(n, x_ref, o_ref, held, send, recv, send_b, recv_b):
    seq, head = lax.axis_index("seq"), lax.axis_index("head")
    targets = others(n, seq)
    greet([(to, head) for to in targets])
    copies = [
        remote(x_ref.at[to], held.at[step], send.at[step], recv.at[step], (to, head))
        for step, to in enumerate(targets)
    ]
    for copy in copies:
        copy.start()
    total = x_ref[seq].astype(jnp.float32)
    for step, copy in enumerate(copies):
        copy.wait()
        total = total + held[step].astype(jnp.float32)
    o_ref[seq] = total.astype(o_ref.dtype)
    copies = [
        remote(o_ref.at[seq], o_ref.at[seq], send_b.at[step], recv_b.at[step], (to, head))
        for step, to in enumerate(targets)
    ]
    for copy in copies:
        copy.start()
    for copy in copies:
        copy.wait()


def seq_sum(x, n):
    dma = pltpu.SemaphoreType.DMA
    return pl.pallas_call(
        functools.partial(sum_kernel, n),
        out_shape=jax.ShapeDtypeStruct(x.shape, x.dtype),
        in_specs=[VMEM],
        out_specs=VMEM,
        scratch_shapes=[
            pltpu.VMEM((n - 1,) + x.shape[1:], x.dtype),
            dma((n - 1,)), dma((n - 1,)), dma((n - 1,)), dma((n - 1,)),
        ],
        compiler_params=comm_params(4),
        name="gradient_sum",
    )(x)


def pick_kernel(index_ref, x_ref, o_ref):
    o_ref[...] = x_ref[...]


def pick_blocks(x, index):
    block = (1,) + x.shape[1:]
    return pl.pallas_call(
        pick_kernel,
        out_shape=jax.ShapeDtypeStruct(index.shape + x.shape[1:], x.dtype),
        grid_spec=pltpu.PrefetchScalarGridSpec(
            num_scalar_prefetch=1,
            grid=index.shape,
            in_specs=[pl.BlockSpec(block, lambda i, index: (index[i], 0, 0))],
            out_specs=pl.BlockSpec(block, lambda i, index: (i, 0, 0)),
        ),
        name="pick_blocks",
    )(index, x)


def encode_kernel(flag_ref, x_ref, w_ref, gain_ref, o_ref, q_ref, k_ref, v_ref, a_ref):
    width = x_ref.shape[1]
    wide = x_ref[...].astype(jnp.float32)
    factor = lax.rsqrt(jnp.mean(wide * wide, axis=-1, keepdims=True) + EPSILON)
    normed = (wide * factor * gain_ref[...]).astype(jnp.bfloat16)

    def project(which):
        return lax.dot_general(
            normed, w_ref[which].reshape(width, width), NT, preferred_element_type=jnp.float32
        ).astype(jnp.bfloat16)

    q_ref[...] = project(0) * jnp.bfloat16(HDIM ** (-0.5))
    k_ref[...] = project(1)
    v_ref[...] = project(2)
    apart = jnp.where(flag_ref[0] > 0, 0.0, -1e30).astype(jnp.float32)
    key_block = lax.broadcasted_iota(jnp.int32, (1, PAIR), 1) // BLK
    first = lax.broadcasted_iota(jnp.int32, (BLK, LANES), 1) < HDIM

    def slab(index, carry):
        columns = pl.ds(pl.multiple_of(index * LANES, LANES), LANES)
        keys = k_ref[:, columns]
        values = v_ref[:, columns]
        for block in range(2):
            rows = pl.ds(block * BLK, BLK)
            bias = jnp.where(key_block == block, 0.0, apart)
            query = q_ref[rows, columns]
            halves = []
            for half in range(2):
                chosen = first if half == 0 else jnp.logical_not(first)
                own = jnp.where(chosen, query, jnp.zeros_like(query))
                scores = lax.dot_general(own, keys, NT, preferred_element_type=jnp.float32) + bias
                top = jnp.max(scores, axis=-1, keepdims=True)
                weights = jnp.exp(scores - top)
                total = jnp.sum(weights, axis=-1, keepdims=True)
                mixed = jnp.dot(
                    weights.astype(jnp.bfloat16), values, preferred_element_type=jnp.float32
                )
                halves.append(mixed * (1.0 / total))
            a_ref[rows, columns] = jnp.where(first, halves[0], halves[1]).astype(jnp.bfloat16)
        return carry

    lax.fori_loop(0, width // LANES, slab, 0)
    mixed = jnp.dot(a_ref[...], w_ref[3].reshape(width, width), preferred_element_type=jnp.float32)
    o_ref[...] = (x_ref[...].astype(jnp.float32) + mixed).astype(jnp.bfloat16)


def encode(flag, rows, weights, gain):
    return pl.pallas_call(
        encode_kernel,
        out_shape=jax.ShapeDtypeStruct(rows.shape, rows.dtype),
        in_specs=[pl.BlockSpec(memory_space=pltpu.SMEM), VMEM, VMEM, VMEM],
        out_specs=VMEM,
        scratch_shapes=[pltpu.VMEM(rows.shape, jnp.bfloat16)] * 4,
        compiler_params=pltpu.CompilerParams(vmem_limit_bytes=56 * 1024 * 1024),
        name="encode_pair",
    )(flag, rows, weights, gain)


def norm_rows(values, gain_vector):
    widened = values.astype(jnp.float32)
    factor = lax.rsqrt(jnp.mean(widened * widened, axis=-1, keepdims=True) + EPSILON)
    return (widened * factor * gain_vector).astype(jnp.bfloat16)


def renorm(updated, initial, axis):
    target_norm = jnp.sqrt(jnp.sum(initial * initial, axis=axis, keepdims=True))
    return (
        updated
        * target_norm
        * lax.rsqrt(jnp.sum(updated * updated, axis=axis, keepdims=True) + EPSILON)
    )


def to_tiles(gradient, n):
    rows, columns = gradient.shape
    flat = jnp.concatenate(
        [gradient[:, c : c + LANES] for c in range(0, columns, LANES)], axis=0
    )
    chunk = 16 * (-(-flat.shape[0] // (16 * n)))
    return jnp.pad(flat, ((0, chunk * n - flat.shape[0]), (0, 0))).reshape(n, chunk, LANES)


def from_tiles(tiles, rows, columns):
    flat = tiles.reshape(-1, LANES)
    return jnp.concatenate(
        [flat[c * rows : (c + 1) * rows] for c in range(columns // LANES)], axis=1
    )


def on_device(
    patches,
    slot_image,
    slot_dest,
    enc_gain,
    w_qkv,
    w_out,
    fast_gain,
    w_fast,
    w_rate,
    fast_gate_up,
    fast_down,
):
    n = lax.axis_size("seq")
    nh = lax.axis_size("head")
    head = lax.axis_index("head")
    width = w_out.shape[0]
    model = patches.shape[1]
    part = PAIR // nh
    shard_pairs = BLK_DEV // 2

    first_dest = slot_dest[0::2]
    same_image = (slot_image[0::2] == slot_image[1::2]).astype(jnp.int32)
    pair_dest = first_dest // 2
    goes = (pair_dest[None, :] // shard_pairs == jnp.arange(n)[:, None]) & (first_dest >= 0)[None, :]
    has = jnp.any(goes, axis=1)
    offset = head * part
    slot = 2 * jnp.arange(first_dest.shape[0]) + (first_dest + offset // BLK) % 2
    start = (slot * BLK + offset % BLK) // part
    send_index = jnp.sum(jnp.where(goes, start[None, :], 0), axis=1).astype(jnp.int32)
    code = jnp.sum(
        jnp.where(goes, (2 * (pair_dest % shard_pairs) + same_image)[None, :], 0), axis=1
    )
    code = jnp.where(has, code, -1).astype(jnp.int32)
    meta = jnp.broadcast_to(code[:, None, None], (n, 8, LANES))
    sending = pick_blocks(patches.reshape(-1, part, model), send_index)
    weights = jnp.concatenate([jnp.swapaxes(w_qkv, 1, 2), w_out[None]], axis=0)
    arrived, codes, full_weights = enter(sending, meta, weights, n, nh)
    codes = codes[:, 0, 0]
    source = (codes[None, :] >= 0) & (codes[None, :] // 2 == jnp.arange(shard_pairs)[:, None])
    source_index = jnp.sum(jnp.where(source, jnp.arange(n)[None, :], 0), axis=1).astype(jnp.int32)
    same = jnp.sum(
        jnp.where((codes >= 0) & (codes // 2 == head), codes % 2, 0)
    ).astype(jnp.int32)
    own_pair = head_swap(pick_blocks(arrived, source_index), nh).reshape(PAIR, model)
    own_embedded = encode(same.reshape(1), own_pair, full_weights, enc_gain[None, :])
    full_embedded = head_gather(own_embedded, nh).reshape(nh * PAIR, model)
    embedded = lax.dynamic_slice_in_dim(full_embedded, head * width, width, 1)

    normed_fast = norm_rows(full_embedded, fast_gain)
    fast_query = jnp.dot(normed_fast, w_fast[0], preferred_element_type=jnp.float32).astype(
        jnp.bfloat16
    )
    fast_key = jnp.dot(normed_fast, w_fast[1], preferred_element_type=jnp.float32).astype(
        jnp.bfloat16
    )
    fast_value = jnp.dot(normed_fast, w_fast[2], preferred_element_type=jnp.float32).astype(
        jnp.bfloat16
    )
    token_total = embedded.shape[0] * n
    rates = (
        RATE_SCALE
        * jax.nn.softplus(jnp.dot(normed_fast, w_rate, preferred_element_type=jnp.float32))
        * token_total ** (-0.5)
    )
    gate_init = fast_gate_up[0, 0]
    up_init = fast_gate_up[0, 1]
    down_init = fast_down[0]
    gate_half = gate_init.astype(jnp.bfloat16)
    up_half = up_init.astype(jnp.bfloat16)
    down_half = down_init.astype(jnp.bfloat16)
    key_gate = jnp.dot(fast_key, gate_half, preferred_element_type=jnp.float32)
    key_up = jnp.dot(fast_key, up_half, preferred_element_type=jnp.float32)
    sigmoid_gate = jax.nn.sigmoid(key_gate)
    hidden_key = (key_gate * sigmoid_gate * key_up).astype(jnp.bfloat16)
    out_grad = (-rates * fast_value.astype(jnp.float32)).astype(jnp.bfloat16)
    grad_down = jnp.einsum("tf,th->fh", out_grad, hidden_key, preferred_element_type=jnp.float32)
    hidden_grad = jnp.dot(out_grad, down_half.T, preferred_element_type=jnp.float32)
    gate_grad = (
        hidden_grad * key_up * sigmoid_gate * (1.0 + key_gate * (1.0 - sigmoid_gate))
    ).astype(jnp.bfloat16)
    up_grad = (hidden_grad * key_gate * sigmoid_gate).astype(jnp.bfloat16)
    grad_gate = jnp.einsum("tf,th->fh", fast_key, gate_grad, preferred_element_type=jnp.float32)
    grad_up = jnp.einsum("tf,th->fh", fast_key, up_grad, preferred_element_type=jnp.float32)
    gradient = jnp.concatenate([grad_gate, grad_up, grad_down], axis=0).astype(jnp.bfloat16)
    hidden = gradient.shape[1]
    summed = from_tiles(seq_sum(to_tiles(gradient, n), n), 3 * width, hidden).astype(jnp.float32)
    new_gate = renorm(gate_init - summed[:width], gate_init, 1)
    new_up = renorm(up_init - summed[width : 2 * width], up_init, 1)
    new_down = renorm(down_init.T - summed[2 * width :], down_init.T, 0)
    applied_gate = new_gate.astype(jnp.bfloat16)
    applied_up = new_up.astype(jnp.bfloat16)
    applied_down = new_down.astype(jnp.bfloat16)
    query_gate = jnp.dot(fast_query, applied_gate, preferred_element_type=jnp.float32)
    query_up = jnp.dot(fast_query, applied_up, preferred_element_type=jnp.float32)
    query_hidden = (jax.nn.silu(query_gate) * query_up).astype(jnp.bfloat16)
    fast_out = jnp.dot(query_hidden, applied_down.T, preferred_element_type=jnp.float32)
    return (embedded.astype(jnp.float32) + fast_out).astype(jnp.bfloat16)


def solution(mesh):
    in_specs = (
        P("seq", None),
        P("seq"),
        P("seq"),
        P(),
        P(None, None, "head"),
        P("head", None),
        P(),
        P(None, None, "head"),
        P(None, "head"),
        P("head", None, None, None),
        P("head", None, None),
    )
    out_specs = P("seq", "head")
    return jax.shard_map(
        on_device, mesh=mesh, in_specs=in_specs, out_specs=out_specs, check_vma=False
    )
```

```python
import functools

import jax
import jax.numpy as jnp
from jax import lax
from jax.experimental import pallas as pl
from jax.experimental.pallas import tpu as pltpu
from jax.sharding import PartitionSpec as P

HDIM = 64
BLK = 256
BLK_DEV = 8
PAIR = 2 * BLK
EPSILON = 1e-06
RATE_SCALE = 0.1
LANES = 128
MESH = pl.DeviceIdType.MESH
VMEM = pl.BlockSpec(memory_space=pltpu.VMEM)
NT = (((1,), (1,)), ((), ()))


def remote(src, dst, send, recv, device):
    return pltpu.make_async_remote_copy(
        src_ref=src, dst_ref=dst, send_sem=send, recv_sem=recv, device_id=device, device_id_type=MESH
    )


def comm_params(number):
    return pltpu.CompilerParams(
        collective_id=number, has_side_effects=True, vmem_limit_bytes=56 * 1024 * 1024
    )


def greet(devices):
    barrier = pltpu.get_barrier_semaphore()
    for device in devices:
        pl.semaphore_signal(barrier, inc=1, device_id=device, device_id_type=MESH)
    pl.semaphore_wait(barrier, len(devices))


def others(axis_size, me):
    return [lax.rem(me + step, axis_size) for step in range(1, axis_size)]


def head_pals(head_count, head):
    partner = head + 1 - 2 * lax.rem(head, 2)
    peer = lax.rem(head + head_count // 2, head_count)
    return partner, peer


def entry_kernel(n, nh, x_ref, m_ref, w_ref, ox, om, ow, sx, rx, sm, rm, sw, rw):
    seq, head = lax.axis_index("seq"), lax.axis_index("head")
    partner, peer = head_pals(nh, head)
    across = lax.rem(partner + nh // 2, nh)
    targets = others(n, seq)
    greet([(seq, partner), (seq, peer)] + [(to, head) for to in targets])
    to_peer = remote(w_ref, ow.at[:, head], sw.at[0], rw.at[0], (seq, peer))
    to_partner = remote(w_ref, ow.at[:, head], sw.at[1], rw.at[1], (seq, partner))
    to_peer.start()
    to_partner.start()
    copies = []
    for step, to in enumerate(targets):
        copies.append(remote(m_ref.at[to], om.at[seq], sm.at[step], rm.at[step], (to, head)))
        copies.append(remote(x_ref.at[to], ox.at[seq], sx.at[step], rx.at[step], (to, head)))
    for copy in copies:
        copy.start()
    ox[seq] = x_ref[seq]
    om[seq] = m_ref[seq]
    for part in range(w_ref.shape[0]):
        ow[part, head] = w_ref[part]
    to_peer.wait_recv()
    forward = remote(ow.at[:, peer], ow.at[:, peer], sw.at[2], rw.at[2], (seq, partner))
    forward.start()
    to_peer.wait_send()
    to_partner.wait()
    for copy in copies:
        copy.wait()
    forward.wait()


def enter(rows, meta, weights, n, nh):
    dma = pltpu.SemaphoreType.DMA
    return pl.pallas_call(
        functools.partial(entry_kernel, n, nh),
        out_shape=(
            jax.ShapeDtypeStruct(rows.shape, rows.dtype),
            jax.ShapeDtypeStruct(meta.shape, meta.dtype),
            jax.ShapeDtypeStruct(
                (weights.shape[0], nh) + weights.shape[1:], weights.dtype
            ),
        ),
        in_specs=[VMEM] * 3,
        out_specs=(VMEM,) * 3,
        scratch_shapes=[
            dma((n - 1,)), dma((n - 1,)), dma((n - 1,)), dma((n - 1,)), dma((3,)), dma((3,)),
        ],
        compiler_params=comm_params(1),
        name="entry_exchange",
    )(rows, meta, weights)


def swap_kernel(nh, x_ref, o_ref, send, recv):
    seq, head = lax.axis_index("seq"), lax.axis_index("head")
    targets = others(nh, head)
    greet([(seq, to) for to in targets])
    copies = [
        remote(x_ref.at[to], o_ref.at[head], send.at[step], recv.at[step], (seq, to))
        for step, to in enumerate(targets)
    ]
    for copy in copies:
        copy.start()
    o_ref[head] = x_ref[head]
    for copy in copies:
        copy.wait()


def head_swap(x, nh):
    dma = pltpu.SemaphoreType.DMA
    return pl.pallas_call(
        functools.partial(swap_kernel, nh),
        out_shape=jax.ShapeDtypeStruct(x.shape, x.dtype),
        in_specs=[VMEM],
        out_specs=VMEM,
        scratch_shapes=[dma((nh - 1,)), dma((nh - 1,))],
        compiler_params=comm_params(2),
        name="head_swap",
    )(x)


def sum_kernel(n, x_ref, o_ref, held, send, recv, send_b, recv_b):
    seq, head = lax.axis_index("seq"), lax.axis_index("head")
    targets = others(n, seq)
    greet([(to, head) for to in targets])
    copies = [
        remote(x_ref.at[to], held.at[step], send.at[step], recv.at[step], (to, head))
        for step, to in enumerate(targets)
    ]
    for copy in copies:
        copy.start()
    total = x_ref[seq].astype(jnp.float32)
    for step, copy in enumerate(copies):
        copy.wait()
        total = total + held[step].astype(jnp.float32)
    o_ref[seq] = total.astype(o_ref.dtype)
    copies = [
        remote(o_ref.at[seq], o_ref.at[seq], send_b.at[step], recv_b.at[step], (to, head))
        for step, to in enumerate(targets)
    ]
    for copy in copies:
        copy.start()
    for copy in copies:
        copy.wait()


def seq_sum(x, n):
    dma = pltpu.SemaphoreType.DMA
    return pl.pallas_call(
        functools.partial(sum_kernel, n),
        out_shape=jax.ShapeDtypeStruct(x.shape, x.dtype),
        in_specs=[VMEM],
        out_specs=VMEM,
        scratch_shapes=[
            pltpu.VMEM((n - 1,) + x.shape[1:], x.dtype),
            dma((n - 1,)), dma((n - 1,)), dma((n - 1,)), dma((n - 1,)),
        ],
        compiler_params=comm_params(4),
        name="gradient_sum",
    )(x)


def route_kernel(nh, dest_ref, image_ref, x_ref, o_ref, m_ref, sems):
    head = lax.axis_index("head")
    part = o_ref.shape[1]
    pairs = dest_ref.shape[0] // 2
    m_ref[...] = jnp.full(m_ref.shape, -1, jnp.int32)

    def piece(pair):
        dest = dest_ref[2 * pair]
        known = jnp.maximum(dest, 0)
        offset = head * part
        slot = 2 * pair + lax.rem(known + lax.div(offset, BLK), 2)
        start = pl.multiple_of(slot * BLK + lax.rem(offset, BLK), part)
        target = lax.div(known, BLK_DEV)
        copy = pltpu.make_async_copy(x_ref.at[pl.ds(start, part)], o_ref.at[target], sems.at[pair])
        return dest, target, copy

    for pair in range(pairs):
        dest, target, copy = piece(pair)

        @pl.when(dest >= 0)
        def _():
            copy.start()
            same = (image_ref[2 * pair] == image_ref[2 * pair + 1]).astype(jnp.int32)
            code = 2 * lax.div(lax.rem(dest, BLK_DEV), 2) + same
            m_ref[target] = jnp.full(m_ref.shape[1:], code, jnp.int32)

    for pair in range(pairs):
        dest, target, copy = piece(pair)

        @pl.when(dest >= 0)
        def _():
            copy.wait()


def route(slot_dest, slot_image, patches, n, nh):
    smem = pl.BlockSpec(memory_space=pltpu.SMEM)
    part = PAIR // nh
    return pl.pallas_call(
        functools.partial(route_kernel, nh),
        out_shape=(
            jax.ShapeDtypeStruct((n, part, patches.shape[1]), patches.dtype),
            jax.ShapeDtypeStruct((n, 8, LANES), jnp.int32),
        ),
        in_specs=[smem, smem, pl.BlockSpec(memory_space=pl.ANY)],
        out_specs=(VMEM, VMEM),
        scratch_shapes=[pltpu.SemaphoreType.DMA((slot_dest.shape[0] // 2,))],
        compiler_params=pltpu.CompilerParams(vmem_limit_bytes=56 * 1024 * 1024),
        name="route_pairs",
    )(slot_dest, slot_image, patches)


def select_kernel(code_ref, x_ref, o_ref, same_ref, sems):
    head = lax.axis_index("head")
    same_ref[0] = 0

    def begin(source, carry):
        code = code_ref[source]

        @pl.when(code >= 0)
        def _():
            pair = lax.div(code, 2)
            pltpu.make_async_copy(x_ref.at[source], o_ref.at[pair], sems.at[pair]).start()

            @pl.when(pair == head)
            def _():
                same_ref[0] = lax.rem(code, 2)

        return carry

    lax.fori_loop(0, code_ref.shape[0], begin, 0)
    for pair in range(o_ref.shape[0]):
        pltpu.make_async_copy(x_ref.at[0], o_ref.at[pair], sems.at[pair]).wait()


def select(codes, arrived, pairs):
    smem = pl.BlockSpec(memory_space=pltpu.SMEM)
    return pl.pallas_call(
        select_kernel,
        out_shape=(
            jax.ShapeDtypeStruct((pairs,) + arrived.shape[1:], arrived.dtype),
            jax.ShapeDtypeStruct((1,), jnp.int32),
        ),
        in_specs=[smem, pl.BlockSpec(memory_space=pl.ANY)],
        out_specs=(VMEM, smem),
        scratch_shapes=[pltpu.SemaphoreType.DMA((pairs,))],
        compiler_params=pltpu.CompilerParams(vmem_limit_bytes=24 * 1024 * 1024),
        name="select_pairs",
    )(codes, arrived)


CHUNK = 128


def encode_kernel(
    nh, flag_ref, x_ref, w_ref, gain_ref, o_ref, q_ref, k_ref, v_ref, a_ref, send, recv
):
    seq, head = lax.axis_index("seq"), lax.axis_index("head")
    partner, peer = head_pals(nh, head)
    greet([(seq, partner), (seq, peer)])
    width = x_ref.shape[1]
    wide = x_ref[...].astype(jnp.float32)
    factor = lax.rsqrt(jnp.mean(wide * wide, axis=-1, keepdims=True) + EPSILON)
    normed = (wide * factor * gain_ref[...]).astype(jnp.bfloat16)

    def project(which):
        return lax.dot_general(
            normed, w_ref[which].reshape(width, width), NT, preferred_element_type=jnp.float32
        ).astype(jnp.bfloat16)

    q_ref[...] = project(0) * jnp.bfloat16(HDIM ** (-0.5))
    k_ref[...] = project(1)
    v_ref[...] = project(2)
    apart = jnp.where(flag_ref[0] > 0, 0.0, -1e30).astype(jnp.float32)
    key_block = lax.broadcasted_iota(jnp.int32, (1, PAIR), 1) // BLK
    first = lax.broadcasted_iota(jnp.int32, (CHUNK, LANES), 1) < HDIM
    direct = []
    forwards = []

    for chunk in range(PAIR // CHUNK):
        rows = pl.ds(chunk * CHUNK, CHUNK)
        bias = jnp.where(key_block == chunk * CHUNK // BLK, 0.0, apart)

        def slabs(index, carry):
            for inner in range(2):
                columns = pl.ds(pl.multiple_of((2 * index + inner) * LANES, LANES), LANES)
                query = q_ref[rows, columns]
                nothing = jnp.zeros_like(query)
                both = jnp.concatenate(
                    [jnp.where(first, query, nothing), jnp.where(first, nothing, query)], axis=0
                )
                scores = lax.dot_general(
                    both, k_ref[:, columns], NT, preferred_element_type=jnp.float32
                ) + bias
                top = jnp.max(scores, axis=-1, keepdims=True)
                weights = jnp.exp(scores - top)
                total = jnp.sum(weights, axis=-1, keepdims=True)
                mixed = jnp.dot(
                    weights.astype(jnp.bfloat16),
                    v_ref[:, columns],
                    preferred_element_type=jnp.float32,
                ) * (1.0 / total)
                a_ref[:, columns] = jnp.where(first, mixed[:CHUNK], mixed[CHUNK:]).astype(
                    jnp.bfloat16
                )
            return carry

        lax.fori_loop(0, width // LANES // 2, slabs, 0)
        mixed = jnp.dot(
            a_ref[...], w_ref[3].reshape(width, width), preferred_element_type=jnp.float32
        )
        o_ref[head, rows] = (x_ref[rows].astype(jnp.float32) + mixed).astype(jnp.bfloat16)
        mine = o_ref.at[head, rows]
        to_peer = remote(mine, mine, send.at[0, chunk], recv.at[0, chunk], (seq, peer))
        to_partner = remote(mine, mine, send.at[1, chunk], recv.at[1, chunk], (seq, partner))
        to_peer.start()
        to_partner.start()
        direct.append((to_peer, to_partner))
    for chunk, (to_peer, to_partner) in enumerate(direct):
        to_peer.wait_recv()
        theirs = o_ref.at[peer, pl.ds(chunk * CHUNK, CHUNK)]
        forward = remote(theirs, theirs, send.at[2, chunk], recv.at[2, chunk], (seq, partner))
        forward.start()
        forwards.append(forward)
    for (to_peer, to_partner), forward in zip(direct, forwards):
        to_peer.wait_send()
        to_partner.wait()
        forward.wait()


def encode_and_gather(flag, rows, weights, gain, nh):
    dma = pltpu.SemaphoreType.DMA
    chunks = PAIR // CHUNK
    return pl.pallas_call(
        functools.partial(encode_kernel, nh),
        out_shape=jax.ShapeDtypeStruct((nh,) + rows.shape, rows.dtype),
        in_specs=[pl.BlockSpec(memory_space=pltpu.SMEM), VMEM, VMEM, VMEM],
        out_specs=VMEM,
        scratch_shapes=[pltpu.VMEM(rows.shape, jnp.bfloat16)] * 3
        + [pltpu.VMEM((CHUNK, rows.shape[1]), jnp.bfloat16), dma((3, chunks)), dma((3, chunks))],
        compiler_params=comm_params(3),
        name="encode_and_gather",
    )(flag, rows, weights, gain)


def norm_rows(values, gain_vector):
    widened = values.astype(jnp.float32)
    factor = lax.rsqrt(jnp.mean(widened * widened, axis=-1, keepdims=True) + EPSILON)
    return (widened * factor * gain_vector).astype(jnp.bfloat16)


def renorm(updated, initial, axis):
    target_norm = jnp.sqrt(jnp.sum(initial * initial, axis=axis, keepdims=True))
    return (
        updated
        * target_norm
        * lax.rsqrt(jnp.sum(updated * updated, axis=axis, keepdims=True) + EPSILON)
    )


def to_tiles(gradient, n):
    rows, columns = gradient.shape
    flat = jnp.concatenate(
        [gradient[:, c : c + LANES] for c in range(0, columns, LANES)], axis=0
    )
    chunk = 16 * (-(-flat.shape[0] // (16 * n)))
    return jnp.pad(flat, ((0, chunk * n - flat.shape[0]), (0, 0))).reshape(n, chunk, LANES)


def from_tiles(tiles, rows, columns):
    flat = tiles.reshape(-1, LANES)
    return jnp.concatenate(
        [flat[c * rows : (c + 1) * rows] for c in range(columns // LANES)], axis=1
    )


def on_device(
    patches,
    slot_image,
    slot_dest,
    enc_gain,
    w_qkv,
    w_out,
    fast_gain,
    w_fast,
    w_rate,
    fast_gate_up,
    fast_down,
):
    n = lax.axis_size("seq")
    nh = lax.axis_size("head")
    head = lax.axis_index("head")
    width = w_out.shape[0]
    model = patches.shape[1]
    sending, meta = route(slot_dest, slot_image, patches, n, nh)
    weights = jnp.concatenate([jnp.swapaxes(w_qkv, 1, 2), w_out[None]], axis=0)
    arrived, codes, full_weights = enter(sending, meta, weights, n, nh)
    chosen, same = select(codes[:, 0, 0], arrived, BLK_DEV // 2)
    own_pair = head_swap(chosen, nh).reshape(PAIR, model)
    full_embedded = encode_and_gather(same, own_pair, full_weights, enc_gain[None, :], nh)
    full_embedded = full_embedded.reshape(nh * PAIR, model)
    embedded = lax.dynamic_slice_in_dim(full_embedded, head * width, width, 1)

    normed_fast = norm_rows(full_embedded, fast_gain)
    fast_query = jnp.dot(normed_fast, w_fast[0], preferred_element_type=jnp.float32).astype(
        jnp.bfloat16
    )
    fast_key = jnp.dot(normed_fast, w_fast[1], preferred_element_type=jnp.float32).astype(
        jnp.bfloat16
    )
    fast_value = jnp.dot(normed_fast, w_fast[2], preferred_element_type=jnp.float32).astype(
        jnp.bfloat16
    )
    token_total = embedded.shape[0] * n
    rates = (
        RATE_SCALE
        * jax.nn.softplus(jnp.dot(normed_fast, w_rate, preferred_element_type=jnp.float32))
        * token_total ** (-0.5)
    )
    gate_init = fast_gate_up[0, 0]
    up_init = fast_gate_up[0, 1]
    down_init = fast_down[0]
    gate_half = gate_init.astype(jnp.bfloat16)
    up_half = up_init.astype(jnp.bfloat16)
    down_half = down_init.astype(jnp.bfloat16)
    key_gate = jnp.dot(fast_key, gate_half, preferred_element_type=jnp.float32)
    key_up = jnp.dot(fast_key, up_half, preferred_element_type=jnp.float32)
    sigmoid_gate = jax.nn.sigmoid(key_gate)
    hidden_key = (key_gate * sigmoid_gate * key_up).astype(jnp.bfloat16)
    out_grad = (-rates * fast_value.astype(jnp.float32)).astype(jnp.bfloat16)
    grad_down = jnp.einsum("tf,th->fh", out_grad, hidden_key, preferred_element_type=jnp.float32)
    hidden_grad = jnp.dot(out_grad, down_half.T, preferred_element_type=jnp.float32)
    gate_grad = (
        hidden_grad * key_up * sigmoid_gate * (1.0 + key_gate * (1.0 - sigmoid_gate))
    ).astype(jnp.bfloat16)
    up_grad = (hidden_grad * key_gate * sigmoid_gate).astype(jnp.bfloat16)
    grad_gate = jnp.einsum("tf,th->fh", fast_key, gate_grad, preferred_element_type=jnp.float32)
    grad_up = jnp.einsum("tf,th->fh", fast_key, up_grad, preferred_element_type=jnp.float32)
    gradient = jnp.concatenate([grad_gate, grad_up, grad_down], axis=0).astype(jnp.bfloat16)
    hidden = gradient.shape[1]
    summed = from_tiles(seq_sum(to_tiles(gradient, n), n), 3 * width, hidden).astype(jnp.float32)
    new_gate = renorm(gate_init - summed[:width], gate_init, 1)
    new_up = renorm(up_init - summed[width : 2 * width], up_init, 1)
    new_down = renorm(down_init.T - summed[2 * width :], down_init.T, 0)
    applied_gate = new_gate.astype(jnp.bfloat16)
    applied_up = new_up.astype(jnp.bfloat16)
    applied_down = new_down.astype(jnp.bfloat16)
    query_gate = jnp.dot(fast_query, applied_gate, preferred_element_type=jnp.float32)
    query_up = jnp.dot(fast_query, applied_up, preferred_element_type=jnp.float32)
    query_hidden = (jax.nn.silu(query_gate) * query_up).astype(jnp.bfloat16)
    fast_out = jnp.dot(query_hidden, applied_down.T, preferred_element_type=jnp.float32)
    return (embedded.astype(jnp.float32) + fast_out).astype(jnp.bfloat16)


def solution(mesh):
    in_specs = (
        P("seq", None),
        P("seq"),
        P("seq"),
        P(),
        P(None, None, "head"),
        P("head", None),
        P(),
        P(None, None, "head"),
        P(None, "head"),
        P("head", None, None, None),
        P("head", None, None),
    )
    out_specs = P("seq", "head")
    return jax.shard_map(
        on_device, mesh=mesh, in_specs=in_specs, out_specs=out_specs, check_vma=False
    )
```
